32 devices in a mesh: groups: 2 (over y), seq: 4 (over z), head: 2 (over x), layer: 2 (over core).
Axes of the slice: x: 2, y: 2, z: 4, core: 2. Of those that a mesh axis runs over, the one named last changes fastest.
Arguments:
- kv_cache: bfloat16 [2, 2, 8, 4096, 2, 128], P(None, 'layer', 'groups', 'seq', 'head'), parts along dimension 2, may hold values from -800 to 800
- valid_blocks: int32 [8], P('groups'), parts along dimension 0, may hold values from 1 to 32, 64 in all
Outputs:
- decode_cache: bfloat16 [2, 2, 8, 4096, 2, 128], P(None, 'layer', ('groups', 'seq'), None, 'head'), parts along dimension 2
- centers: float32 [2, 2, 8, 2, 128], P(None, 'layer', 'groups', 'head'), parts along dimension 2
- scales: float32 [2, 2, 8, 2, 128], P(None, 'layer', 'groups', 'head'), parts along dimension 2
The draws below stay inside these ranges and needn't reach their ends.
There are 2 independent parts, one for each index of `groups`. The reference program is written for one: setup_inputs(seed, part) draws one part's arguments, and reference() takes and returns one part's arrays. A program takes and returns all parts, laid end to end along the dimension named above; each array names one. Nothing has to cross between parts.
Inputs may be any that keep to these rules, and one draw needn't show every extreme that they name: `valid_blocks`: the counts of the 4 users sum to 64, and the largest equals 32.
All inputs are finite; a program needn't handle non-finite values.
Results may differ from the reference program's by a relative error of at most 0.001.
Values may be sent and summed in bfloat16 or wider, within the bound.
A program may use at most 64 MiB of HBM per device.

```python
import math
import jax
import jax.numpy as jnp
import numpy as np

HEAD = 128
KVH = 2
LAYERS = 2
USERS = 4
PDEV = 1024
BLOCK = 128
SEQ = 4096
NBLK = 32
N_SEQ = 4


def draw_kv_cache(key, part):
    shape = (2, LAYERS, USERS, SEQ, KVH, HEAD)
    row_shape = (2, LAYERS, USERS, SEQ, KVH, 1)
    col_shape = (2, LAYERS, USERS, 1, KVH, HEAD)
    keys = jax.random.split(jax.random.fold_in(key, 11), 4)
    cols = jnp.exp(jax.random.uniform(keys[1], col_shape, jnp.float32, 0.0, math.log(10.0)))
    trend = 1.0 + 2.0 * jnp.arange(SEQ, dtype=jnp.float32).reshape(1, 1, 1, SEQ, 1, 1) / SEQ
    rows = jnp.exp(jax.random.uniform(keys[0], row_shape, jnp.float32, 0.0, math.log(10.0)))
    noise = jnp.clip(jax.random.normal(keys[2], shape, jnp.float32), -4.0, 4.0)
    offset = jnp.clip(jax.random.normal(keys[3], col_shape, jnp.float32), -4.0, 4.0) * 3.0 * cols
    value = trend * (offset + 0.3 * rows * cols * noise)
    return value.astype(jnp.bfloat16)


def split_up(amount, total, reach, skew):
    portions = [(1 << 20) // math.isqrt(standing ** skew) + 1 for standing in range(2, amount + 1)]
    spare, counts = total - reach - (amount - 1), [1] * (amount - 1)
    while spare > 0:
        candidates = [i for i in range(amount - 1) if counts[i] < reach]
        pool, remaining = sum([portions[i] for i in candidates]), spare
        for i in candidates:
            more = min(reach - counts[i], max(1, remaining * portions[i] // pool), spare)
            counts[i] = counts[i] + more
            spare = spare - more
    return np.array([reach] + counts)


def uneven_parts(key, count, total, limit, lean):
    if count == 2:
        one = jax.random.randint(key, (), max(1, total - limit), min(limit, total - 1) + 1)
        return jnp.stack([one, total - one])
    sizes = jnp.asarray(split_up(count, total, limit, lean), jnp.int32)
    pairs = (count - 1) // 2
    donor, sink = sizes[1:1 + 2 * pairs:2], sizes[2:2 + 2 * pairs:2]
    margin = jnp.minimum(donor - 1, limit - sink)
    shifted = jax.random.randint(jax.random.fold_in(key, 1), (pairs,), 0, 1 << 20) % (margin + 1)
    sizes = sizes.at[1:1 + 2 * pairs:2].set(donor - shifted).at[2:2 + 2 * pairs:2].set(sink + shifted)
    return sizes[jax.random.permutation(jax.random.fold_in(key, 2), count)]


def setup_inputs(seed: int = 0, part: int = 0) -> dict:
    key_list = jax.random.split(jax.random.key(seed), 3)
    part_keys = jax.random.split(jax.random.fold_in(key_list[2], part), 3)
    return {
        "kv_cache": draw_kv_cache(jax.random.fold_in(jax.random.fold_in(key_list[2], part), 71), part),
        "valid_blocks": uneven_parts(part_keys[1], USERS, USERS * NBLK // 2, NBLK, 2).astype(jnp.int32),
    }


epsilon = 1e-6


def reference(kv_cache, valid_blocks):
    lengths = valid_blocks.astype(jnp.int32) * BLOCK
    values = kv_cache.astype(jnp.float32)
    position = jnp.arange(SEQ, dtype=jnp.int32)
    is_live = position[None, :] < lengths[:, None]
    live_mask = is_live[None, None, :, :, None, None]
    totals = jnp.sum(jnp.where(live_mask, values, 0.0), axis=3)
    centers = totals / lengths.astype(jnp.float32)[None, None, :, None, None]
    spread = jnp.max(jnp.where(live_mask, jnp.abs(values - centers[:, :, :, None]), 0.0), axis=3)
    scales = spread + epsilon
    normed = jnp.where(live_mask, (values - centers[:, :, :, None]) / scales[:, :, :, None], 0.0).astype(jnp.bfloat16)
    owns = N_SEQ // USERS
    slice_len = PDEV // owns
    shaped = normed.reshape(2, LAYERS, USERS, N_SEQ, owns, slice_len, KVH, HEAD)
    shaped = jnp.transpose(shaped, (0, 1, 2, 4, 3, 5, 6, 7))
    decode_cache = shaped.reshape(2, LAYERS, USERS * owns, N_SEQ * slice_len, KVH, HEAD)
    return decode_cache, centers, scales
```

```python
import functools

import jax
import jax.numpy as jnp
from jax import lax
from jax.experimental import pallas as pl
from jax.experimental.pallas import tpu as pltpu
from jax.sharding import PartitionSpec as P

BLOCK = 128
ROWS = 8
GRANT = 16 * 2**20
EPSILON = 1e-06


def transport(n, quarter, blocks_ref, kv_ref, recv_ref, stats_ref, local, load_sem, own_sem,
              send_sem, recv_sem, stat_send, stat_recv):
    kinds, users, per_dev, width = kv_ref.shape
    part = per_dev // quarter
    me = lax.axis_index("seq")

    load = pltpu.make_async_copy(kv_ref, local, load_sem)
    load.start()

    barrier = pltpu.get_barrier_semaphore()
    for d in range(n):
        @pl.when(me != d)
        def _():
            pl.semaphore_signal(barrier, inc=1, device_id={"seq": d})
    pl.semaphore_wait(barrier, n - 1)

    def bulk(source, target, k):
        user, q = target // quarter, target % quarter
        return pltpu.make_async_remote_copy(
            src_ref=kv_ref.at[k, user, pl.ds(pl.multiple_of(q * part, part), part), :],
            dst_ref=recv_ref.at[k, pl.ds(pl.multiple_of(source * part, part), part), :],
            send_sem=send_sem.at[target, k],
            recv_sem=recv_sem.at[source, k],
            device_id={"seq": target},
        )

    def stat(source, target):
        return pltpu.make_async_remote_copy(
            src_ref=stats_ref.at[source],
            dst_ref=stats_ref.at[source],
            send_sem=stat_send.at[target],
            recv_sem=stat_recv.at[source],
            device_id={"seq": target},
        )

    def start_bulk(dist):
        for k in range(kinds):
            @pl.when(me + dist < n)
            def _():
                bulk(me, me + dist, k).start()

            @pl.when(me - dist >= 0)
            def _():
                bulk(me, me - dist, k).start()

    start_bulk(1)
    own = pltpu.make_async_copy(
        kv_ref.at[:, me // quarter, pl.ds(pl.multiple_of((me % quarter) * part, part), part), :],
        recv_ref.at[:, pl.ds(pl.multiple_of(me * part, part), part), :],
        own_sem,
    )
    own.start()
    load.wait()

    count = per_dev // BLOCK
    for k in range(kinds):
        for u in range(users):
            live = blocks_ref[u] - me * count

            def step(b, carry, k=k, u=u, live=live):
                total, high, low = carry
                x = local[k, u, pl.ds(pl.multiple_of(b * BLOCK, BLOCK), BLOCK), :].astype(jnp.float32)
                x = x.reshape(BLOCK // ROWS, ROWS, width)
                on = b < live
                total = total + jnp.where(on, jnp.sum(x, axis=0), 0.0)
                high = jnp.maximum(high, jnp.where(on, jnp.max(x, axis=0), -jnp.inf))
                low = jnp.minimum(low, jnp.where(on, jnp.min(x, axis=0), jnp.inf))
                return total, high, low

            shape = (ROWS, width)
            total, high, low = lax.fori_loop(
                0, count, step,
                (jnp.zeros(shape, jnp.float32), jnp.full(shape, -jnp.inf, jnp.float32),
                 jnp.full(shape, jnp.inf, jnp.float32)),
            )
            stats_ref[me, 0, k, u, :] = jnp.sum(total, axis=0)
            stats_ref[me, 1, k, u, :] = jnp.max(high, axis=0)
            stats_ref[me, 2, k, u, :] = jnp.min(low, axis=0)

    for d in range(n):
        @pl.when(me != d)
        def _():
            stat(me, d).start()
    for dist in range(2, n):
        start_bulk(dist)

    own.wait()
    for s in range(n):
        @pl.when(me != s)
        def _():
            stat(me, s).wait_send()
            stat(s, me).wait_recv()
            for k in range(kinds):
                bulk(me, s, k).wait_send()
                bulk(s, me, k).wait_recv()


def finish(n, quarter, chunk, blocks_ref, recv_ref, stats_ref, out_ref, centers_ref, scales_ref,
           inverse, ready, out_sem):
    _, _, kinds, users, width = stats_ref.shape
    positions = recv_ref.shape[1]
    part = positions // n
    me = lax.axis_index("seq")
    for u in range(users):
        length = (blocks_ref[u] * BLOCK).astype(jnp.float32)
        for k in range(kinds):
            total = stats_ref[0, 0, k, u, :]
            high, low = stats_ref[0, 1, k, u, :], stats_ref[0, 2, k, u, :]
            for s in range(1, n):
                total = total + stats_ref[s, 0, k, u, :]
                high = jnp.maximum(high, stats_ref[s, 1, k, u, :])
                low = jnp.minimum(low, stats_ref[s, 2, k, u, :])
            center = total / jnp.full_like(total, length)
            scale = jnp.maximum(high - center, center - low) + EPSILON
            centers_ref[k, u, :] = center
            scales_ref[k, u, :] = scale
            inverse[k, u, :] = 1.0 / scale

    user = me // quarter
    length = blocks_ref[user] * BLOCK
    per_part = part // chunk
    per_dev = part * quarter
    base = (me % quarter) * part
    iota = lax.broadcasted_iota(jnp.int32, (chunk, width), 0)
    for k in range(kinds):
        center = centers_ref[k, pl.ds(user, 1), :]
        scale = inverse[k, pl.ds(user, 1), :]

        def step(i, _, k=k, center=center, scale=scale):
            rows = pl.ds(pl.multiple_of(i * chunk, chunk), chunk)
            first = (i // per_part) * per_dev + base + (i % per_part) * chunk
            x = recv_ref[k, rows, :].astype(jnp.float32)
            y = jnp.where(first + iota < length, (x - center) * scale, 0.0)
            ready[k, rows, :] = y.astype(jnp.bfloat16)
            pltpu.make_async_copy(ready.at[k, rows, :], out_ref.at[k, rows, :],
                                  out_sem.at[k, i]).start()
            return 0

        lax.fori_loop(0, positions // chunk, step, 0)
    for k in range(kinds):
        def done(i, _, k=k):
            rows = pl.ds(pl.multiple_of(i * chunk, chunk), chunk)
            pltpu.make_async_copy(ready.at[k, rows, :], out_ref.at[k, rows, :],
                                  out_sem.at[k, i]).wait()
            return 0

        lax.fori_loop(0, positions // chunk, done, 0)


def on_device(kv_cache, valid_blocks):
    kind_count, layer_dev, user_count, per_dev, heads_dev, width = kv_cache.shape
    n = lax.axis_size("seq")
    quarter = n // user_count
    part = per_dev // quarter
    kinds = kind_count * layer_dev * heads_dev
    kv = jnp.transpose(kv_cache, (0, 1, 4, 2, 3, 5)).reshape(kinds, user_count, per_dev, width)
    vmem = pl.BlockSpec(memory_space=pltpu.VMEM)
    smem = pl.BlockSpec(memory_space=pltpu.SMEM)
    anywhere = pl.BlockSpec(memory_space=pl.ANY)
    recv, stats = pl.pallas_call(
        functools.partial(transport, n, quarter),
        out_shape=(
            jax.ShapeDtypeStruct((kinds, n * part, width), jnp.bfloat16),
            jax.ShapeDtypeStruct((n, 3, kinds, user_count, width), jnp.float32),
        ),
        in_specs=[smem, anywhere],
        out_specs=(vmem, vmem),
        scratch_shapes=[
            pltpu.VMEM((kinds, user_count, per_dev, width), jnp.bfloat16),
            pltpu.SemaphoreType.DMA,
            pltpu.SemaphoreType.DMA,
            pltpu.SemaphoreType.DMA((n, kinds)),
            pltpu.SemaphoreType.DMA((n, kinds)),
            pltpu.SemaphoreType.DMA((n,)),
            pltpu.SemaphoreType.DMA((n,)),
        ],
        compiler_params=pltpu.CompilerParams(
            collective_id=0, has_side_effects=True, vmem_limit_bytes=GRANT
        ),
        name="transport",
    )(valid_blocks, kv)
    chunk = min(part, 512)
    small = jax.ShapeDtypeStruct((kinds, user_count, width), jnp.float32)
    out, centers, scales = pl.pallas_call(
        functools.partial(finish, n, quarter, chunk),
        out_shape=(jax.ShapeDtypeStruct((kinds, n * part, width), jnp.bfloat16), small, small),
        in_specs=[smem, vmem, vmem],
        out_specs=(anywhere, vmem, vmem),
        scratch_shapes=[
            pltpu.VMEM((kinds, user_count, width), jnp.float32),
            pltpu.VMEM((kinds, n * part, width), jnp.bfloat16),
            pltpu.SemaphoreType.DMA((kinds, n * part // chunk)),
        ],
        compiler_params=pltpu.CompilerParams(vmem_limit_bytes=GRANT),
        name="finish",
    )(valid_blocks, recv, stats)

    def spread(x, middle):
        x = x.reshape(kind_count, layer_dev, heads_dev, *middle, width)
        return jnp.moveaxis(x, 2, -2)

    return (
        spread(out, (1, n * part)),
        spread(centers, (user_count,)),
        spread(scales, (user_count,)),
    )


def solution(mesh):
    in_specs = (P(None, "layer", "groups", "seq", "head", None), P("groups"))
    out_specs = (
        P(None, "layer", ("groups", "seq"), None, "head", None),
        P(None, "layer", "groups", "head", None),
        P(None, "layer", "groups", "head", None),
    )
    return jax.shard_map(
        on_device, mesh=mesh, in_specs=in_specs, out_specs=out_specs, check_vma=False
    )
```

```python
import functools

import jax
import jax.numpy as jnp
from jax import lax
from jax.experimental import pallas as pl
from jax.experimental.pallas import tpu as pltpu
from jax.sharding import PartitionSpec as P

BLOCK = 128
ROWS = 8
CHUNK = 256
GRANT = 16 * 2**20
EPSILON = 1e-06


def normalised(recv_ref, k, rows, first, length, center, inverse):
    x = recv_ref[k, rows, :].astype(jnp.float32)
    position = first + lax.broadcasted_iota(jnp.int32, x.shape, 0)
    return jnp.where(position < length, (x - center) * inverse, 0.0).astype(jnp.bfloat16)


def last_source(me, n):
    return jnp.where(me < n - 1 - me, n - 1, 0)


def transport(n, quarter, chunk, blocks_ref, kv_ref, recv_ref, stats_ref, centers_ref, scales_ref,
              inverse_ref, blocks, local, load_sem, blocks_sem, own_sem, send_sem, recv_sem,
              stat_send, stat_recv):
    kinds, users, per_dev, width = kv_ref.shape
    part = per_dev // quarter
    me = lax.axis_index("seq")

    load = pltpu.make_async_copy(kv_ref, local, load_sem)
    load.start()
    fetch = pltpu.make_async_copy(blocks_ref, blocks, blocks_sem)
    fetch.start()

    barrier = pltpu.get_barrier_semaphore()
    for d in range(n):
        @pl.when(me != d)
        def _():
            pl.semaphore_signal(barrier, inc=1, device_id={"seq": d})
    pl.semaphore_wait(barrier, n - 1)

    def bulk(source, target, k):
        user, q = target // quarter, target % quarter
        return pltpu.make_async_remote_copy(
            src_ref=kv_ref.at[k, user, pl.ds(pl.multiple_of(q * part, part), part), :],
            dst_ref=recv_ref.at[k, pl.ds(pl.multiple_of(source * part, part), part), :],
            send_sem=send_sem.at[target, k],
            recv_sem=recv_sem.at[source, k],
            device_id={"seq": target},
        )

    def stat(source, target):
        return pltpu.make_async_remote_copy(
            src_ref=stats_ref.at[source],
            dst_ref=stats_ref.at[source],
            send_sem=stat_send.at[target],
            recv_sem=stat_recv.at[source],
            device_id={"seq": target},
        )

    def start_bulk(dist):
        for k in range(kinds):
            @pl.when(me + dist < n)
            def _():
                bulk(me, me + dist, k).start()

            @pl.when(me - dist >= 0)
            def _():
                bulk(me, me - dist, k).start()

    start_bulk(1)
    own = pltpu.make_async_copy(
        kv_ref.at[:, me // quarter, pl.ds(pl.multiple_of((me % quarter) * part, part), part), :],
        recv_ref.at[:, pl.ds(pl.multiple_of(me * part, part), part), :],
        own_sem,
    )
    own.start()
    fetch.wait()
    load.wait()

    count = per_dev // BLOCK
    for k in range(kinds):
        for u in range(users):
            live = blocks[u] - me * count

            def step(b, carry, k=k, u=u, live=live):
                total, high, low = carry
                x = local[k, u, pl.ds(pl.multiple_of(b * BLOCK, BLOCK), BLOCK), :].astype(jnp.float32)
                x = x.reshape(BLOCK // ROWS, ROWS, width)
                on = b < live
                total = total + jnp.where(on, jnp.sum(x, axis=0), 0.0)
                high = jnp.maximum(high, jnp.where(on, jnp.max(x, axis=0), -jnp.inf))
                low = jnp.minimum(low, jnp.where(on, jnp.min(x, axis=0), jnp.inf))
                return total, high, low

            shape = (ROWS, width)
            total, high, low = lax.fori_loop(
                0, count, step,
                (jnp.zeros(shape, jnp.float32), jnp.full(shape, -jnp.inf, jnp.float32),
                 jnp.full(shape, jnp.inf, jnp.float32)),
            )
            stats_ref[me, 0, k, u, :] = jnp.sum(total, axis=0)
            stats_ref[me, 1, k, u, :] = jnp.max(high, axis=0)
            stats_ref[me, 2, k, u, :] = jnp.min(low, axis=0)

    for d in range(n):
        @pl.when(me != d)
        def _():
            stat(me, d).start()
    for dist in range(2, n):
        start_bulk(dist)

    for s in range(n):
        @pl.when(me != s)
        def _():
            stat(s, me).wait_recv()
    for u in range(users):
        length = (blocks[u] * BLOCK).astype(jnp.float32)
        for k in range(kinds):
            total = stats_ref[0, 0, k, u, :]
            high, low = stats_ref[0, 1, k, u, :], stats_ref[0, 2, k, u, :]
            for s in range(1, n):
                total = total + stats_ref[s, 0, k, u, :]
                high = jnp.maximum(high, stats_ref[s, 1, k, u, :])
                low = jnp.minimum(low, stats_ref[s, 2, k, u, :])
            center = total / jnp.full_like(total, length)
            scale = jnp.maximum(high - center, center - low) + EPSILON
            centers_ref[k, u, :] = center
            scales_ref[k, u, :] = scale
            inverse_ref[k, u, :] = 1.0 / scale

    user = me // quarter
    base = (me % quarter) * part
    length = jnp.zeros((1, width), jnp.int32)
    for u in range(users):
        length = jnp.where(user == u, blocks[u] * BLOCK, length)

    def normalise(source, k):
        center = centers_ref[k, pl.ds(user, 1), :]
        inverse = inverse_ref[k, pl.ds(user, 1), :]

        def step(i, _):
            rows = pl.ds(pl.multiple_of(source * part + i * chunk, chunk), chunk)
            first = source * per_dev + base + i * chunk
            recv_ref[k, rows, :] = normalised(recv_ref, k, rows, first, length, center, inverse)
            return 0

        lax.fori_loop(0, part // chunk, step, 0)

    own.wait()
    for k in range(kinds):
        normalise(me, k)
    last = last_source(me, n)
    for dist in range(1, n):
        for source, inside in ((me + dist, me + dist < n), (me - dist, me - dist >= 0)):
            for k in range(kinds):
                @pl.when(inside & (source != last))
                def _():
                    bulk(source, me, k).wait_recv()
                    normalise(source, k)
    for k in range(kinds):
        bulk(last, me, k).wait_recv()
    for s in range(n):
        @pl.when(me != s)
        def _():
            stat(me, s).wait_send()
            for k in range(kinds):
                bulk(me, s, k).wait_send()


def finish(n, quarter, chunk, blocks_ref, recv_ref, c_ref, s_ref, i_ref, out_ref, centers_ref,
           scales_ref, ready, out_sem, ready_sem):
    kinds, positions, width = recv_ref.shape
    part = positions // n
    me = lax.axis_index("seq")
    last = last_source(me, n)

    def place(s, k):
        rows = pl.ds(pl.multiple_of(s * part, part), part)
        return pltpu.make_async_copy(recv_ref.at[k, rows, :], out_ref.at[k, rows, :],
                                     out_sem.at[s, k])

    for s in range(n):
        @pl.when(s != last)
        def _():
            for k in range(kinds):
                place(s, k).start()

    user = me // quarter
    length = blocks_ref[user] * BLOCK
    first = last * part * quarter + (me % quarter) * part
    steps = part // chunk

    def late(k, i):
        return pltpu.make_async_copy(
            ready.at[k, pl.ds(i * chunk, chunk), :],
            out_ref.at[k, pl.ds(pl.multiple_of(last * part + i * chunk, chunk), chunk), :],
            ready_sem.at[k, i],
        )

    for k in range(kinds):
        center = c_ref[k, pl.ds(user, 1), :]
        inverse = i_ref[k, pl.ds(user, 1), :]
        for i in range(steps):
            rows = pl.ds(pl.multiple_of(last * part + i * chunk, chunk), chunk)
            ready[k, pl.ds(i * chunk, chunk), :] = normalised(
                recv_ref, k, rows, first + i * chunk, length, center, inverse
            )
            late(k, i).start()
    centers_ref[...] = c_ref[...]
    scales_ref[...] = s_ref[...]
    for k in range(kinds):
        for i in range(steps):
            late(k, i).wait()
    for s in range(n):
        @pl.when(s != last)
        def _():
            for k in range(kinds):
                place(s, k).wait()


def on_device(kv_cache, valid_blocks):
    kind_count, layer_dev, user_count, per_dev, heads_dev, width = kv_cache.shape
    n = lax.axis_size("seq")
    quarter = n // user_count
    part = per_dev // quarter
    kinds = kind_count * layer_dev * heads_dev
    kv = jnp.transpose(kv_cache, (0, 1, 4, 2, 3, 5)).reshape(kinds, user_count, per_dev, width)
    kv = pltpu.with_memory_space_constraint(kv, pltpu.HBM)
    blocks = pltpu.with_memory_space_constraint(valid_blocks, pltpu.HBM)
    vmem = pl.BlockSpec(memory_space=pltpu.VMEM)
    smem = pl.BlockSpec(memory_space=pltpu.SMEM)
    anywhere = pl.BlockSpec(memory_space=pl.ANY)
    hbm = pl.BlockSpec(memory_space=pltpu.HBM)
    chunk = min(part, CHUNK)
    small = jax.ShapeDtypeStruct((kinds, user_count, width), jnp.float32)
    recv, _, centers, scales, inverse = pl.pallas_call(
        functools.partial(transport, n, quarter, chunk),
        out_shape=(
            jax.ShapeDtypeStruct((kinds, n * part, width), jnp.bfloat16),
            jax.ShapeDtypeStruct((n, 3, kinds, user_count, width), jnp.float32),
            small,
            small,
            small,
        ),
        in_specs=[hbm, hbm],
        out_specs=(vmem,) * 5,
        scratch_shapes=[
            pltpu.SMEM((user_count,), jnp.int32),
            pltpu.VMEM((kinds, user_count, per_dev, width), jnp.bfloat16),
            pltpu.SemaphoreType.DMA,
            pltpu.SemaphoreType.DMA,
            pltpu.SemaphoreType.DMA,
            pltpu.SemaphoreType.DMA((n, kinds)),
            pltpu.SemaphoreType.DMA((n, kinds)),
            pltpu.SemaphoreType.DMA((n,)),
            pltpu.SemaphoreType.DMA((n,)),
        ],
        compiler_params=pltpu.CompilerParams(
            collective_id=0, has_side_effects=True, vmem_limit_bytes=GRANT
        ),
        name="transport",
    )(blocks, kv)
    out, centers, scales = pl.pallas_call(
        functools.partial(finish, n, quarter, chunk),
        out_shape=(jax.ShapeDtypeStruct((kinds, n * part, width), jnp.bfloat16), small, small),
        in_specs=[smem, vmem, vmem, vmem, vmem],
        out_specs=(anywhere, vmem, vmem),
        scratch_shapes=[
            pltpu.VMEM((kinds, part, width), jnp.bfloat16),
            pltpu.SemaphoreType.DMA((n, kinds)),
            pltpu.SemaphoreType.DMA((kinds, part // chunk)),
        ],
        compiler_params=pltpu.CompilerParams(vmem_limit_bytes=GRANT),
        name="finish",
    )(valid_blocks, recv, centers, scales, inverse)

    def spread(x, middle):
        x = x.reshape(kind_count, layer_dev, heads_dev, *middle, width)
        return jnp.moveaxis(x, 2, -2)

    return (
        spread(out, (1, n * part)),
        spread(centers, (user_count,)),
        spread(scales, (user_count,)),
    )


def solution(mesh):
    in_specs = (P(None, "layer", "groups", "seq", "head", None), P("groups"))
    out_specs = (
        P(None, "layer", ("groups", "seq"), None, "head", None),
        P(None, "layer", "groups", "head", None),
        P(None, "layer", "groups", "head", None),
    )
    return jax.shard_map(
        on_device, mesh=mesh, in_specs=in_specs, out_specs=out_specs, check_vma=False
    )
```

```python
import functools

import jax
import jax.numpy as jnp
from jax import lax
from jax.experimental import pallas as pl
from jax.experimental.pallas import tpu as pltpu
from jax.sharding import PartitionSpec as P

BLOCK = 128
ROWS = 8
CHUNK = 256
GRANT = 16 * 2**20
EPSILON = 1e-06


def normalised(recv_ref, k, rows, first, length, center, inverse):
    x = recv_ref[k, rows, :].astype(jnp.float32)
    position = first + lax.broadcasted_iota(jnp.int32, x.shape, 0)
    return jnp.where(position < length, (x - center) * inverse, 0.0).astype(jnp.bfloat16)


def last_source(me, n):
    return jnp.where(me < n - 1 - me, n - 1, 0)


def transport(n, quarter, chunk, blocks_ref, kv_ref, recv_ref, stats_ref, centers_ref, scales_ref,
              inverse_ref, blocks, local, load_sem, blocks_sem, own_sem, send_sem, recv_sem,
              stat_send, stat_recv, entered):
    kinds, users, per_dev, width = kv_ref.shape
    part = per_dev // quarter
    me = lax.axis_index("seq")

    load = pltpu.make_async_copy(kv_ref, local, load_sem)
    load.start()
    fetch = pltpu.make_async_copy(blocks_ref, blocks, blocks_sem)
    fetch.start()

    barrier = pltpu.get_barrier_semaphore()
    has_right, has_left = me + 1 < n, me >= 1

    @pl.when(has_right)
    def _():
        pl.semaphore_signal(barrier, inc=1, device_id={"seq": me + 1})

    @pl.when(has_left)
    def _():
        pl.semaphore_signal(barrier, inc=1, device_id={"seq": me - 1})

    pl.semaphore_wait(barrier, has_right.astype(jnp.int32) + has_left.astype(jnp.int32))

    def bulk(source, target, k, origin=kv_ref):
        user, q = target // quarter, target % quarter
        return pltpu.make_async_remote_copy(
            src_ref=origin.at[k, user, pl.ds(pl.multiple_of(q * part, part), part), :],
            dst_ref=recv_ref.at[k, pl.ds(pl.multiple_of(source * part, part), part), :],
            send_sem=send_sem.at[target, k],
            recv_sem=recv_sem.at[source, k],
            device_id={"seq": target},
        )

    def stat(source, target):
        return pltpu.make_async_remote_copy(
            src_ref=stats_ref.at[source],
            dst_ref=stats_ref.at[source],
            send_sem=stat_send.at[target],
            recv_sem=stat_recv.at[source],
            device_id={"seq": target},
        )

    def start_bulk(dist, origin):
        for k in range(kinds):
            @pl.when(me + dist < n)
            def _():
                bulk(me, me + dist, k, origin).start()

            @pl.when(me - dist >= 0)
            def _():
                bulk(me, me - dist, k, origin).start()

    start_bulk(1, kv_ref)
    own = pltpu.make_async_copy(
        kv_ref.at[:, me // quarter, pl.ds(pl.multiple_of((me % quarter) * part, part), part), :],
        recv_ref.at[:, pl.ds(pl.multiple_of(me * part, part), part), :],
        own_sem,
    )
    own.start()

    for dist in range(2, n):
        @pl.when(has_right & (me - (dist - 1) >= 0))
        def _():
            pl.semaphore_signal(entered.at[0, dist], inc=1, device_id={"seq": me + 1})

        @pl.when(has_left & (me + (dist - 1) < n))
        def _():
            pl.semaphore_signal(entered.at[1, dist], inc=1, device_id={"seq": me - 1})

        @pl.when(me - dist >= 0)
        def _():
            pl.semaphore_wait(entered.at[0, dist], 1)

        @pl.when(me + dist < n)
        def _():
            pl.semaphore_wait(entered.at[1, dist], 1)

    fetch.wait()
    load.wait()

    count = per_dev // BLOCK
    for k in range(kinds):
        for u in range(users):
            live = blocks[u] - me * count

            def step(b, carry, k=k, u=u, live=live):
                total, high, low = carry
                x = local[k, u, pl.ds(pl.multiple_of(b * BLOCK, BLOCK), BLOCK), :].astype(jnp.float32)
                x = x.reshape(BLOCK // ROWS, ROWS, width)
                on = b < live
                total = total + jnp.where(on, jnp.sum(x, axis=0), 0.0)
                high = jnp.maximum(high, jnp.where(on, jnp.max(x, axis=0), -jnp.inf))
                low = jnp.minimum(low, jnp.where(on, jnp.min(x, axis=0), jnp.inf))
                return total, high, low

            shape = (ROWS, width)
            total, high, low = lax.fori_loop(
                0, count, step,
                (jnp.zeros(shape, jnp.float32), jnp.full(shape, -jnp.inf, jnp.float32),
                 jnp.full(shape, jnp.inf, jnp.float32)),
            )
            stats_ref[me, 0, k, u, :] = jnp.sum(total, axis=0)
            stats_ref[me, 1, k, u, :] = jnp.max(high, axis=0)
            stats_ref[me, 2, k, u, :] = jnp.min(low, axis=0)

    for d in range(n):
        @pl.when(me != d)
        def _():
            stat(me, d).start()
    for dist in range(n - 1, 1, -1):
        start_bulk(dist, local)

    for s in range(n):
        @pl.when(me != s)
        def _():
            stat(s, me).wait_recv()
    for u in range(users):
        length = (blocks[u] * BLOCK).astype(jnp.float32)
        for k in range(kinds):
            total = stats_ref[0, 0, k, u, :]
            high, low = stats_ref[0, 1, k, u, :], stats_ref[0, 2, k, u, :]
            for s in range(1, n):
                total = total + stats_ref[s, 0, k, u, :]
                high = jnp.maximum(high, stats_ref[s, 1, k, u, :])
                low = jnp.minimum(low, stats_ref[s, 2, k, u, :])
            center = total / jnp.full_like(total, length)
            scale = jnp.maximum(high - center, center - low) + EPSILON
            centers_ref[k, u, :] = center
            scales_ref[k, u, :] = scale
            inverse_ref[k, u, :] = 1.0 / scale

    user = me // quarter
    base = (me % quarter) * part
    length = jnp.zeros((1, width), jnp.int32)
    for u in range(users):
        length = jnp.where(user == u, blocks[u] * BLOCK, length)

    def normalise(source, k):
        center = centers_ref[k, pl.ds(user, 1), :]
        inverse = inverse_ref[k, pl.ds(user, 1), :]

        def step(i, _):
            rows = pl.ds(pl.multiple_of(source * part + i * chunk, chunk), chunk)
            first = source * per_dev + base + i * chunk
            recv_ref[k, rows, :] = normalised(recv_ref, k, rows, first, length, center, inverse)
            return 0

        lax.fori_loop(0, part // chunk, step, 0)

    own.wait()
    for k in range(kinds):
        normalise(me, k)
    last = last_source(me, n)
    for dist in (1, *range(n - 1, 1, -1)):
        for source, inside in ((me + dist, me + dist < n), (me - dist, me - dist >= 0)):
            for k in range(kinds):
                @pl.when(inside & (source != last))
                def _():
                    bulk(source, me, k).wait_recv()
                    normalise(source, k)
    for k in range(kinds):
        bulk(last, me, k).wait_recv()
    for s in range(n):
        @pl.when(me != s)
        def _():
            stat(me, s).wait_send()
            for k in range(kinds):
                bulk(me, s, k).wait_send()


def finish(n, quarter, chunk, blocks_ref, recv_ref, c_ref, s_ref, i_ref, out_ref, centers_ref,
           scales_ref, ready, out_sem, ready_sem):
    kinds, positions, width = recv_ref.shape
    part = positions // n
    me = lax.axis_index("seq")
    last = last_source(me, n)

    def place(s, k):
        rows = pl.ds(pl.multiple_of(s * part, part), part)
        return pltpu.make_async_copy(recv_ref.at[k, rows, :], out_ref.at[k, rows, :],
                                     out_sem.at[s, k])

    for s in range(n):
        @pl.when(s != last)
        def _():
            for k in range(kinds):
                place(s, k).start()

    user = me // quarter
    length = blocks_ref[user] * BLOCK
    first = last * part * quarter + (me % quarter) * part
    steps = part // chunk

    def late(k, i):
        return pltpu.make_async_copy(
            ready.at[k, pl.ds(i * chunk, chunk), :],
            out_ref.at[k, pl.ds(pl.multiple_of(last * part + i * chunk, chunk), chunk), :],
            ready_sem.at[k, i],
        )

    for k in range(kinds):
        center = c_ref[k, pl.ds(user, 1), :]
        inverse = i_ref[k, pl.ds(user, 1), :]
        for i in range(steps):
            rows = pl.ds(pl.multiple_of(last * part + i * chunk, chunk), chunk)
            ready[k, pl.ds(i * chunk, chunk), :] = normalised(
                recv_ref, k, rows, first + i * chunk, length, center, inverse
            )
            late(k, i).start()
    centers_ref[...] = c_ref[...]
    scales_ref[...] = s_ref[...]
    for k in range(kinds):
        for i in range(steps):
            late(k, i).wait()
    for s in range(n):
        @pl.when(s != last)
        def _():
            for k in range(kinds):
                place(s, k).wait()


def on_device(kv_cache, valid_blocks):
    kind_count, layer_dev, user_count, per_dev, heads_dev, width = kv_cache.shape
    n = lax.axis_size("seq")
    quarter = n // user_count
    part = per_dev // quarter
    kinds = kind_count * layer_dev * heads_dev
    kv = jnp.transpose(kv_cache, (0, 1, 4, 2, 3, 5)).reshape(kinds, user_count, per_dev, width)
    kv = pltpu.with_memory_space_constraint(kv, pltpu.HBM)
    blocks = pltpu.with_memory_space_constraint(valid_blocks, pltpu.HBM)
    vmem = pl.BlockSpec(memory_space=pltpu.VMEM)
    smem = pl.BlockSpec(memory_space=pltpu.SMEM)
    anywhere = pl.BlockSpec(memory_space=pl.ANY)
    hbm = pl.BlockSpec(memory_space=pltpu.HBM)
    chunk = min(part, CHUNK)
    small = jax.ShapeDtypeStruct((kinds, user_count, width), jnp.float32)
    recv, _, centers, scales, inverse = pl.pallas_call(
        functools.partial(transport, n, quarter, chunk),
        out_shape=(
            jax.ShapeDtypeStruct((kinds, n * part, width), jnp.bfloat16),
            jax.ShapeDtypeStruct((n, 3, kinds, user_count, width), jnp.float32),
            small,
            small,
            small,
        ),
        in_specs=[hbm, hbm],
        out_specs=(vmem,) * 5,
        scratch_shapes=[
            pltpu.SMEM((user_count,), jnp.int32),
            pltpu.VMEM((kinds, user_count, per_dev, width), jnp.bfloat16),
            pltpu.SemaphoreType.DMA,
            pltpu.SemaphoreType.DMA,
            pltpu.SemaphoreType.DMA,
            pltpu.SemaphoreType.DMA((n, kinds)),
            pltpu.SemaphoreType.DMA((n, kinds)),
            pltpu.SemaphoreType.DMA((n,)),
            pltpu.SemaphoreType.DMA((n,)),
            pltpu.SemaphoreType.REGULAR((2, n)),
        ],
        compiler_params=pltpu.CompilerParams(
            collective_id=0, has_side_effects=True, vmem_limit_bytes=GRANT
        ),
        name="transport",
    )(blocks, kv)
    out, centers, scales = pl.pallas_call(
        functools.partial(finish, n, quarter, chunk),
        out_shape=(jax.ShapeDtypeStruct((kinds, n * part, width), jnp.bfloat16), small, small),
        in_specs=[smem, vmem, vmem, vmem, vmem],
        out_specs=(anywhere, vmem, vmem),
        scratch_shapes=[
            pltpu.VMEM((kinds, part, width), jnp.bfloat16),
            pltpu.SemaphoreType.DMA((n, kinds)),
            pltpu.SemaphoreType.DMA((kinds, part // chunk)),
        ],
        compiler_params=pltpu.CompilerParams(vmem_limit_bytes=GRANT),
        name="finish",
    )(valid_blocks, recv, centers, scales, inverse)

    def spread(x, middle):
        x = x.reshape(kind_count, layer_dev, heads_dev, *middle, width)
        return jnp.moveaxis(x, 2, -2)

    return (
        spread(out, (1, n * part)),
        spread(centers, (user_count,)),
        spread(scales, (user_count,)),
    )


def solution(mesh):
    in_specs = (P(None, "layer", "groups", "seq", "head", None), P("groups"))
    out_specs = (
        P(None, "layer", ("groups", "seq"), None, "head", None),
        P(None, "layer", "groups", "head", None),
        P(None, "layer", "groups", "head", None),
    )
    return jax.shard_map(
        on_device, mesh=mesh, in_specs=in_specs, out_specs=out_specs, check_vma=False
    )
```

```python
import functools

import jax
import jax.numpy as jnp
from jax import lax
from jax.experimental import pallas as pl
from jax.experimental.pallas import tpu as pltpu
from jax.sharding import PartitionSpec as P

BLOCK = 128
ROWS = 8
CHUNK = 256
GRANT = 16 * 2**20
EPSILON = 1e-06


def normalised(recv_ref, k, rows, first, length, center, inverse):
    x = recv_ref[k, rows, :].astype(jnp.float32)
    position = first + lax.broadcasted_iota(jnp.int32, x.shape, 0)
    return jnp.where(position < length, (x - center) * inverse, 0.0).astype(jnp.bfloat16)


def last_source(me, n):
    return jnp.where(me < n - 1 - me, n - 1, 0)


def transport(n, quarter, chunk, blocks_ref, kv_ref, recv_ref, centers_ref, scales_ref,
              inverse_ref, length_ref, stats_ref, blocks, local, load_sem, blocks_sem, own_sem, send_sem, recv_sem,
              stat_send, stat_recv):
    kinds, users, per_dev, width = kv_ref.shape
    part = per_dev // quarter
    me = lax.axis_index("seq")

    load = pltpu.make_async_copy(kv_ref, local, load_sem)
    load.start()
    fetch = pltpu.make_async_copy(blocks_ref, blocks, blocks_sem)
    fetch.start()

    barrier = pltpu.get_barrier_semaphore()
    for d in range(n):
        @pl.when(me != d)
        def _():
            pl.semaphore_signal(barrier, inc=1, device_id={"seq": d})
    pl.semaphore_wait(barrier, n - 1)

    def bulk(source, target, k):
        user, q = target // quarter, target % quarter
        return pltpu.make_async_remote_copy(
            src_ref=kv_ref.at[k, user, pl.ds(pl.multiple_of(q * part, part), part), :],
            dst_ref=recv_ref.at[k, pl.ds(pl.multiple_of(source * part, part), part), :],
            send_sem=send_sem.at[target, k],
            recv_sem=recv_sem.at[source, k],
            device_id={"seq": target},
        )

    def stat(source, target):
        return pltpu.make_async_remote_copy(
            src_ref=stats_ref.at[source],
            dst_ref=stats_ref.at[source],
            send_sem=stat_send.at[target],
            recv_sem=stat_recv.at[source],
            device_id={"seq": target},
        )

    def start_bulk(dist):
        for k in range(kinds):
            @pl.when(me + dist < n)
            def _():
                bulk(me, me + dist, k).start()

            @pl.when(me - dist >= 0)
            def _():
                bulk(me, me - dist, k).start()

    start_bulk(1)
    own = pltpu.make_async_copy(
        kv_ref.at[:, me // quarter, pl.ds(pl.multiple_of((me % quarter) * part, part), part), :],
        recv_ref.at[:, pl.ds(pl.multiple_of(me * part, part), part), :],
        own_sem,
    )
    own.start()
    fetch.wait()
    load.wait()

    count = per_dev // BLOCK
    for k in range(kinds):
        for u in range(users):
            live = blocks[u] - me * count

            def step(b, carry, k=k, u=u, live=live):
                total, high, low = carry
                x = local[k, u, pl.ds(pl.multiple_of(b * BLOCK, BLOCK), BLOCK), :].astype(jnp.float32)
                x = x.reshape(BLOCK // ROWS, ROWS, width)
                on = b < live
                total = total + jnp.where(on, jnp.sum(x, axis=0), 0.0)
                high = jnp.maximum(high, jnp.where(on, jnp.max(x, axis=0), -jnp.inf))
                low = jnp.minimum(low, jnp.where(on, jnp.min(x, axis=0), jnp.inf))
                return total, high, low

            shape = (ROWS, width)
            total, high, low = lax.fori_loop(
                0, count, step,
                (jnp.zeros(shape, jnp.float32), jnp.full(shape, -jnp.inf, jnp.float32),
                 jnp.full(shape, jnp.inf, jnp.float32)),
            )
            stats_ref[me, 0, k, u, :] = jnp.sum(total, axis=0)
            stats_ref[me, 1, k, u, :] = jnp.max(high, axis=0)
            stats_ref[me, 2, k, u, :] = jnp.min(low, axis=0)

    for d in range(n):
        @pl.when(me != d)
        def _():
            stat(me, d).start()
    for dist in range(2, n):
        start_bulk(dist)

    for s in range(n):
        @pl.when(me != s)
        def _():
            stat(s, me).wait_recv()
    for u in range(users):
        length = (blocks[u] * BLOCK).astype(jnp.float32)
        for k in range(kinds):
            total = stats_ref[0, 0, k, u, :]
            high, low = stats_ref[0, 1, k, u, :], stats_ref[0, 2, k, u, :]
            for s in range(1, n):
                total = total + stats_ref[s, 0, k, u, :]
                high = jnp.maximum(high, stats_ref[s, 1, k, u, :])
                low = jnp.minimum(low, stats_ref[s, 2, k, u, :])
            center = total / jnp.full_like(total, length)
            scale = jnp.maximum(high - center, center - low) + EPSILON
            centers_ref[k, u, :] = center
            scales_ref[k, u, :] = scale
            inverse_ref[k, u, :] = 1.0 / scale

    user = me // quarter
    base = (me % quarter) * part
    length = jnp.zeros((1, width), jnp.int32)
    for u in range(users):
        length = jnp.where(user == u, blocks[u] * BLOCK, length)

    length_ref[...] = length

    def normalise(source, k):
        center = centers_ref[k, pl.ds(user, 1), :]
        inverse = inverse_ref[k, pl.ds(user, 1), :]

        def step(i, _):
            rows = pl.ds(pl.multiple_of(source * part + i * chunk, chunk), chunk)
            first = source * per_dev + base + i * chunk
            recv_ref[k, rows, :] = normalised(recv_ref, k, rows, first, length, center, inverse)
            return 0

        lax.fori_loop(0, part // chunk, step, 0)

    own.wait()
    for k in range(kinds):
        normalise(me, k)
    last = last_source(me, n)
    for dist in range(1, n):
        for source, inside in ((me + dist, me + dist < n), (me - dist, me - dist >= 0)):
            for k in range(kinds):
                @pl.when(inside & (source != last))
                def _():
                    bulk(source, me, k).wait_recv()
                    normalise(source, k)
    for k in range(kinds):
        bulk(last, me, k).wait_recv()
    for s in range(n):
        @pl.when(me != s)
        def _():
            stat(me, s).wait_send()
            for k in range(kinds):
                bulk(me, s, k).wait_send()


def finish(n, quarter, chunk, length_ref, recv_ref, c_ref, s_ref, i_ref, out_ref, centers_ref,
           scales_ref, ready, out_sem, ready_sem, small_sem):
    kinds, positions, width = recv_ref.shape
    part = positions // n
    me = lax.axis_index("seq")
    last = last_source(me, n)

    def place(s, k):
        rows = pl.ds(pl.multiple_of(s * part, part), part)
        return pltpu.make_async_copy(recv_ref.at[k, rows, :], out_ref.at[k, rows, :],
                                     out_sem.at[s, k])

    for s in range(n):
        @pl.when(s != last)
        def _():
            for k in range(kinds):
                place(s, k).start()

    small = [
        pltpu.make_async_copy(c_ref, centers_ref, small_sem.at[0]),
        pltpu.make_async_copy(s_ref, scales_ref, small_sem.at[1]),
    ]
    for copy in small:
        copy.start()

    user = me // quarter
    length = length_ref[...]
    first = last * part * quarter + (me % quarter) * part
    steps = part // chunk

    def late(k, i):
        return pltpu.make_async_copy(
            ready.at[k, pl.ds(i * chunk, chunk), :],
            out_ref.at[k, pl.ds(pl.multiple_of(last * part + i * chunk, chunk), chunk), :],
            ready_sem.at[k, i],
        )

    for k in range(kinds):
        center = c_ref[k, pl.ds(user, 1), :]
        inverse = i_ref[k, pl.ds(user, 1), :]
        for i in range(steps):
            rows = pl.ds(pl.multiple_of(last * part + i * chunk, chunk), chunk)
            ready[k, pl.ds(i * chunk, chunk), :] = normalised(
                recv_ref, k, rows, first + i * chunk, length, center, inverse
            )
            late(k, i).start()
    for copy in small:
        copy.wait()
    for k in range(kinds):
        for i in range(steps):
            late(k, i).wait()
    for s in range(n):
        @pl.when(s != last)
        def _():
            for k in range(kinds):
                place(s, k).wait()


def on_device(kv_cache, valid_blocks):
    kind_count, layer_dev, user_count, per_dev, heads_dev, width = kv_cache.shape
    n = lax.axis_size("seq")
    quarter = n // user_count
    part = per_dev // quarter
    kinds = kind_count * layer_dev * heads_dev
    kv = jnp.transpose(kv_cache, (0, 1, 4, 2, 3, 5)).reshape(kinds, user_count, per_dev, width)
    kv = pltpu.with_memory_space_constraint(kv, pltpu.HBM)
    blocks = pltpu.with_memory_space_constraint(valid_blocks, pltpu.HBM)
    vmem = pl.BlockSpec(memory_space=pltpu.VMEM)
    smem = pl.BlockSpec(memory_space=pltpu.SMEM)
    anywhere = pl.BlockSpec(memory_space=pl.ANY)
    hbm = pl.BlockSpec(memory_space=pltpu.HBM)
    chunk = min(part, CHUNK)
    small = jax.ShapeDtypeStruct((kinds, user_count, width), jnp.float32)
    recv, centers, scales, inverse, length = pl.pallas_call(
        functools.partial(transport, n, quarter, chunk),
        out_shape=(
            jax.ShapeDtypeStruct((kinds, n * part, width), jnp.bfloat16),
            small,
            small,
            small,
            jax.ShapeDtypeStruct((1, width), jnp.int32),
        ),
        in_specs=[hbm, hbm],
        out_specs=(vmem,) * 5,
        scratch_shapes=[
            pltpu.VMEM((n, 3, kinds, user_count, width), jnp.float32),
            pltpu.SMEM((user_count,), jnp.int32),
            pltpu.VMEM((kinds, user_count, per_dev, width), jnp.bfloat16),
            pltpu.SemaphoreType.DMA,
            pltpu.SemaphoreType.DMA,
            pltpu.SemaphoreType.DMA,
            pltpu.SemaphoreType.DMA((n, kinds)),
            pltpu.SemaphoreType.DMA((n, kinds)),
            pltpu.SemaphoreType.DMA((n,)),
            pltpu.SemaphoreType.DMA((n,)),
        ],
        compiler_params=pltpu.CompilerParams(
            collective_id=0, has_side_effects=True, vmem_limit_bytes=GRANT
        ),
        name="transport",
    )(blocks, kv)
    out, centers, scales = pl.pallas_call(
        functools.partial(finish, n, quarter, chunk),
        out_shape=(jax.ShapeDtypeStruct((kinds, n * part, width), jnp.bfloat16), small, small),
        in_specs=[vmem] * 5,
        out_specs=(anywhere, anywhere, anywhere),
        scratch_shapes=[
            pltpu.VMEM((kinds, part, width), jnp.bfloat16),
            pltpu.SemaphoreType.DMA((n, kinds)),
            pltpu.SemaphoreType.DMA((kinds, part // chunk)),
            pltpu.SemaphoreType.DMA((2,)),
        ],
        compiler_params=pltpu.CompilerParams(vmem_limit_bytes=GRANT),
        name="finish",
    )(length, recv, centers, scales, inverse)

    def spread(x, middle):
        x = x.reshape(kind_count, layer_dev, heads_dev, *middle, width)
        return jnp.moveaxis(x, 2, -2)

    return (
        spread(out, (1, n * part)),
        spread(centers, (user_count,)),
        spread(scales, (user_count,)),
    )


def solution(mesh):
    in_specs = (P(None, "layer", "groups", "seq", "head", None), P("groups"))
    out_specs = (
        P(None, "layer", ("groups", "seq"), None, "head", None),
        P(None, "layer", "groups", "head", None),
        P(None, "layer", "groups", "head", None),
    )
    return jax.shard_map(
        on_device, mesh=mesh, in_specs=in_specs, out_specs=out_specs, check_vma=False
    )
```
